32 devices in a mesh: gx: 2 (over x), gy: 4 (over z), gz: 4 (over y, core).
Axes of the slice: x: 2, y: 2, z: 4, core: 2. Of those that a mesh axis runs over, the one named last changes fastest.
Arguments:
- particle_mass: float32 [1048576], P(('gx', 'gy', 'gz')), may hold values from 0.5 to 2
- particle_velocity: float32 [3, 1048576], P(None, ('gx', 'gy', 'gz')), may hold values from -6 to 6
- particle_affine: float32 [9, 1048576], P(None, ('gx', 'gy', 'gz')), may hold values from -6 to 6
- particle_cell: int32 [3, 1048576], P(None, ('gx', 'gy', 'gz')), may hold values from 0 to 13
- particle_fraction: int32 [3, 1048576], P(None, ('gx', 'gy', 'gz')), may hold values from 0 to 1023
- block_owner: int32 [2048, 1], P(('gx', 'gy', 'gz')), may hold values from 0 to 15; in each aligned block of 64 rows (0 to 63, 64 to 127, ...) at most 8 rows name the same one
- block_slot: int32 [2048], P(('gx', 'gy', 'gz')), may hold values from 0 to 31
- block_count: int32 [2048], P(('gx', 'gy', 'gz')), may hold values from 128 to 512
- cell_drag: float32 [1024, 4096], P(('gx', 'gy', 'gz')), may hold values from 0.5 to 2
Outputs:
- grid_velocity: float32 [1024, 3, 4096], P(('gx', 'gy', 'gz'))
- new_velocity: float32 [3, 1048576], P(None, ('gx', 'gy', 'gz'))
- new_affine: float32 [9, 1048576], P(None, ('gx', 'gy', 'gz'))
The draws below stay inside these ranges and needn't reach their ends.
Inputs may be any that keep to these rules, and one draw needn't show every extreme that they name: `block_owner`: owner index counted over the devices with the particle device's own gx index, in gy+gz order; among the rows of one device, no owner is named more than 8 times. `block_count`: slots at or beyond the count are absent. `particle_cell`: A particle's three stencil nodes lie inside its grid block.
All inputs are finite; a program needn't handle non-finite values.
Results may differ from the reference program's by a relative error of at most 0.0085.
Values may be sent and summed in bfloat16 or wider, within the bound.
A program may use at most 128 MiB of HBM per device.

```python
import math
import jax
import jax.numpy as jnp
import numpy as np
from jax import lax

EDGE = 16
PB = 512
QUANT = 1024
BLK_DEV = 64
GROUP = 16
CAP = 8
TILES_DEV = 32
BLOCKS = 2048
PARTICLES = 1048576
TILES = 1024
CELLS = 4096
N_GY = 4
N_GZ = 4


def place_ends(entries, key, smallest, high):
    longest = entries.shape.index(max(entries.shape))
    spots = []
    for shift in (0, 1):
        where = [jax.random.randint(jax.random.fold_in(key, axis), (), 0, length) for axis, length in enumerate(entries.shape)]
        where[longest] = (where[longest] + shift) % entries.shape[longest]
        spots.append(tuple(where))
    return entries.at[spots[0]].set(smallest).at[spots[1]].set(high)


def block_levels(own_key, dims, shards, low, largest):
    def one(axis_at, blocks):
        heights = jax.random.uniform(jax.random.fold_in(jax.random.fold_in(own_key, 6), axis_at), (blocks,), jnp.float32, low / len(shards), largest / len(shards))
        return jnp.repeat(jnp.exp(heights), dims[axis_at] // blocks).reshape((-1,) + (1,) * (len(dims) - axis_at - 1))

    loudness = one(*shards[0])
    for cut in shards[1:]:
        loudness = loudness * one(*cut)
    return loudness


def shared_out(stream_key, own, number, rows, amount, top, most, slope):
    order = jax.random.permutation(stream_key, amount)
    packed, common = load_shares(amount, rows * top, most, slope, True), load_shares(amount, rows * top, most, slope, False)
    places = jnp.arange(amount)

    def named(lengths, rotation):
        used = int((lengths > 0).sum())
        fixed = max(1, used // 4)
        shifted = fixed + (places - fixed + rotation * (used - fixed)) % max(1, amount - fixed)
        return jnp.zeros((amount,), jnp.int32).at[order[jnp.where(places < fixed, places, shifted)]].set(jnp.asarray(lengths, jnp.int32))

    lengths = jnp.where(number % 4 == 0, named(packed, number // 4), named(common, number - number // 4 - 1))
    mixed = jax.random.permutation(jax.random.fold_in(own, 3), amount)
    giver, receiver = mixed[0:amount // 2 * 2:2], mixed[1:amount // 2 * 2:2]
    margin = jnp.minimum(lengths[giver] - 1, most - lengths[receiver]) // 2
    margin = jnp.where((giver == order[0]) | (receiver == order[0]) | (lengths[receiver] == 0), 0, jnp.maximum(margin, 0))
    shifted = jax.random.randint(jax.random.fold_in(own, 4), (amount // 2,), 0, 1 << 20) % (margin + 1)
    lengths = lengths.at[giver].add(-shifted).at[receiver].add(shifted)
    labels = jnp.searchsorted(jnp.cumsum(lengths), jnp.arange(rows * top), side="right").astype(jnp.int32)
    table = labels.reshape(top, rows).T
    table = table[jax.random.permutation(jax.random.fold_in(own, 1), rows)]
    rotation = jax.random.randint(jax.random.fold_in(own, 2), (rows, 1), 0, top)
    return jnp.take_along_axis(table, (jnp.arange(top)[None, :] + rotation) % top, axis=1)


def load_shares(amount, total, bound, slope, full):
    loads = [(1 << 20) // math.isqrt(standing ** slope) + 1 for standing in range(1, amount + 1)]
    largest = bound if full else min(bound, max(-(-total // amount), total * loads[0] // sum(loads)))
    least = 1 if total - largest >= amount - 1 else 0
    holding, rest = [largest] + [least] * (amount - 1), total - largest - least * (amount - 1)
    while rest > 0:
        free = [i for i in range(1, amount) if holding[i] < largest] or [i for i in range(1, amount) if holding[i] < bound]
        whole, budget = sum([loads[i] for i in free]), rest
        for i in free:
            more = min(bound - holding[i], max(1, budget * loads[i] // whole), rest)
            holding[i] = holding[i] + more
            rest = rest - more
    return np.array(holding)


def gaussian(stream_key, extent, deviation, reach, pieces=(), kind=jnp.bfloat16):
    result = deviation * jax.random.normal(stream_key, extent, jnp.float32)
    if pieces:
        result = result * block_levels(stream_key, extent, pieces, -0.22, 0.18)
    return jnp.clip(result, -reach, reach).astype(kind)


def setup_inputs(seed: int = 0) -> dict:
    keys = jax.random.split(jax.random.key(seed), 10)
    particle_mass = jnp.clip(jnp.exp(math.log(2.0) - 1.3862944 * jax.random.uniform(keys[0], (PARTICLES,), jnp.float32) ** block_levels(keys[0], (PARTICLES,), ((0, 32),), -0.2, 0.2)), 0.5, 2.0)
    particle_velocity = gaussian(keys[1], (3, PARTICLES), 1.0, 6.0, ((1, 32),), jnp.float32)
    particle_affine = gaussian(keys[2], (9, PARTICLES), 1.0, 6.0, ((1, 32),), jnp.float32)
    particle_cell = place_ends(jax.random.randint(keys[3], (3, PARTICLES), 0, EDGE - 2), jax.random.fold_in(keys[3], 1), 0, (EDGE - 2) - 1).astype(jnp.int32)
    particle_fraction = place_ends(jax.random.randint(keys[4], (3, PARTICLES), 0, QUANT), jax.random.fold_in(keys[4], 1), 0, QUANT - 1).astype(jnp.int32)
    block_owner_keys = jax.random.split(jax.random.fold_in(keys[5], 1), BLOCKS // BLK_DEV)
    block_owner_turns = jax.random.permutation(jax.random.fold_in(keys[5], 3), BLOCKS // BLK_DEV)
    block_owner = jax.vmap(lambda own, number: shared_out(jax.random.fold_in(keys[5], 2), own, number, BLK_DEV, GROUP, 1, CAP, 2))(block_owner_keys, block_owner_turns).reshape((BLOCKS, 1))
    block_slot = place_ends(jax.random.randint(keys[6], (BLOCKS,), 0, TILES_DEV), jax.random.fold_in(keys[6], 1), 0, TILES_DEV - 1).astype(jnp.int32)
    block_count = place_ends(jax.random.randint(keys[7], (BLOCKS,), PB // 4, PB + 1), jax.random.fold_in(keys[7], 1), PB // 4, PB).astype(jnp.int32)
    cell_drag = jnp.clip(jnp.exp(math.log(2.0) - 1.3862944 * jax.random.uniform(keys[8], (TILES, CELLS), jnp.float32) ** block_levels(keys[8], (TILES, CELLS), ((0, 32),), -0.2, 0.2)), 0.5, 2.0)
    return dict(particle_mass=particle_mass, particle_velocity=particle_velocity, particle_affine=particle_affine, particle_cell=particle_cell, particle_fraction=particle_fraction, block_owner=block_owner, block_slot=block_slot, block_count=block_count, cell_drag=cell_drag)


def spline(offset):
    magnitude = jnp.abs(offset)
    inner_part = 0.75 - magnitude * magnitude
    outer_part = 0.5 * (1.5 - magnitude) * (1.5 - magnitude)
    return jnp.where(magnitude < 0.5, inner_part, jnp.where(magnitude < 1.5, outer_part, 0.0))


def particle_table(particle_mass, particle_velocity, particle_affine, particle_cell, particle_fraction, block_count):
    blocks = block_count.shape[0]
    batch_shape = (blocks, particle_mass.shape[0] // blocks)
    places = jnp.arange(batch_shape[1], dtype=jnp.int32)
    present = places[None, :] < block_count[:, None]
    live_mass = jnp.where(present, particle_mass.reshape(batch_shape), 0.0)
    position = particle_cell.astype(jnp.float32) + 0.5 + (particle_fraction.astype(jnp.float32) + 0.5) / QUANT
    return jnp.concatenate([live_mass[None], particle_velocity.reshape((3,) + batch_shape), particle_affine.reshape((9,) + batch_shape), position.reshape((3,) + batch_shape)], axis=0)


def stencil(particle_data):
    node_coords = jnp.arange(EDGE, dtype=jnp.float32)
    offset = node_coords[None, :, None, None] - particle_data[13:16][:, None]
    weights = spline(offset)
    return weights, weights * offset


def planes(weights, slopes):
    def outer(first_factor, second_factor):
        product_table = first_factor[:, None] * second_factor[None, :]
        return product_table.reshape((EDGE * EDGE,) + product_table.shape[2:]).astype(jnp.bfloat16)
    return outer(weights[1], weights[2]), outer(slopes[1], weights[2]), outer(weights[1], slopes[2])


def deposit(particle_data):
    batch_shape = particle_data.shape[1:]
    weights, slopes = stencil(particle_data)
    plane_zero, plane_one, plane_two = planes(weights, slopes)
    live_mass = particle_data[0]
    along_x = weights[0]
    slope_x = slopes[0]
    affine = particle_data[4:13].reshape((3, 3) + batch_shape)
    mass_lead = (live_mass[None] * along_x)[None]
    momentum_lead = live_mass[None, None] * (particle_data[1:4][:, None] * along_x[None] + affine[:, 0][:, None] * slope_x[None])
    lead_zero = jnp.concatenate([mass_lead, momentum_lead], axis=0).astype(jnp.bfloat16)
    lead_one = (live_mass[None, None] * affine[:, 1][:, None] * along_x[None]).astype(jnp.bfloat16)
    lead_two = (live_mass[None, None] * affine[:, 2][:, None] * along_x[None]).astype(jnp.bfloat16)

    def contract(lead, plane):
        flattened = lead.reshape((-1,) + batch_shape).astype(jnp.float32)
        return jnp.einsum("anp,bnp->nab", flattened, plane.astype(jnp.float32), precision=lax.Precision.HIGHEST)

    count_blocks = batch_shape[0]
    dep_zero = contract(lead_zero, plane_zero).reshape(count_blocks, 4, -1)
    dep_one = contract(lead_one, plane_one).reshape(count_blocks, 3, -1)
    dep_two = contract(lead_two, plane_two).reshape(count_blocks, 3, -1)
    return jnp.concatenate([dep_zero[:, :1], dep_zero[:, 1:] + dep_one + dep_two], axis=1)


def interpolate(particle_data, grid_rows):
    batch_shape = particle_data.shape[1:]
    weights, slopes = stencil(particle_data)
    plane_zero, plane_one, plane_two = planes(weights, slopes)
    along_x = weights[0]
    slope_x = slopes[0]
    flattened = grid_rows.reshape(batch_shape[0], 3 * EDGE, EDGE * EDGE).astype(jnp.float32)

    def contract(plane):
        moment = jnp.einsum("nab,bnp->anp", flattened, plane.astype(jnp.float32), precision=lax.Precision.HIGHEST)
        return moment.reshape((3, EDGE) + batch_shape)

    moment_zero = contract(plane_zero)
    moment_one = contract(plane_one)
    moment_two = contract(plane_two)
    velocity_out = jnp.sum(along_x[None] * moment_zero, axis=1)
    column_zero = 4.0 * jnp.sum(slope_x[None] * moment_zero, axis=1)
    column_one = 4.0 * jnp.sum(along_x[None] * moment_one, axis=1)
    column_two = 4.0 * jnp.sum(along_x[None] * moment_two, axis=1)
    affine_out = jnp.stack([column_zero, column_one, column_two], axis=1).reshape((9,) + batch_shape)
    present = (particle_data[0] > 0.0).astype(jnp.float32)
    return jnp.concatenate([velocity_out, affine_out], axis=0) * present[None]


def reference(particle_mass, particle_velocity, particle_affine, particle_cell, particle_fraction, block_owner, block_slot, block_count, cell_drag):
    group_size = N_GY * N_GZ
    particle_data = particle_table(particle_mass, particle_velocity, particle_affine, particle_cell, particle_fraction, block_count)
    blocks = block_count.shape[0]
    device = jnp.arange(blocks, dtype=jnp.int32) // BLK_DEV
    tile_ids = (((device // group_size) * group_size + block_owner[:, 0]) * TILES_DEV + block_slot).astype(jnp.int32)

    def accumulate(grid_sums, block_index):
        portion = lax.dynamic_slice_in_dim(particle_data, block_index, 1, 1)
        return grid_sums.at[tile_ids[block_index]].add(deposit(portion)[0]), None

    initial = jnp.zeros((cell_drag.shape[0], 4, cell_drag.shape[1]), jnp.float32)
    grid_sums = lax.scan(accumulate, initial, jnp.arange(blocks, dtype=jnp.int32))[0]
    grid_velocity = grid_sums[:, 1:] / (grid_sums[:, :1] + cell_drag[:, None, :])
    rounded = grid_velocity.astype(jnp.bfloat16)

    def sample(block_index):
        portion = lax.dynamic_slice_in_dim(particle_data, block_index, 1, 1)
        cell_rows = lax.dynamic_index_in_dim(rounded, tile_ids[block_index], 0, keepdims=True)
        return interpolate(portion, cell_rows)[:, 0]

    finished = lax.map(sample, jnp.arange(blocks, dtype=jnp.int32))
    finished = jnp.transpose(finished, (1, 0, 2)).reshape(12, -1)
    return grid_velocity, finished[:3], finished[3:]
```

```python
import functools

import jax
import jax.numpy as jnp
from jax import lax
from jax.experimental import pallas as pl
from jax.experimental.pallas import tpu as pltpu
from jax.sharding import PartitionSpec as P

EDGE = 16
QUANT = 1024
LANES = 128
FIELDS = 16
RESULTS = 12
PARTS = 4
GROUP_AXES = ("gy", "gz")
F32 = jnp.float32
BF16 = jnp.bfloat16
MESH = pl.DeviceIdType.MESH


SMEM = pl.BlockSpec(memory_space=pltpu.SMEM)
VMEM = pl.BlockSpec(memory_space=pltpu.VMEM)
HBM = pl.BlockSpec(memory_space=pltpu.HBM)


def cost(flops):
    return pl.CostEstimate(flops=flops, bytes_accessed=1 << 22, transcendentals=0)


def plan_kernel(
    cap, owner_ref, slot_ref, count_ref, table_ref, live_ref, dest_ref, marks_ref, used_ref, tile_ref
):
    group = used_ref.shape[0]

    def clear_used(i, carry):
        used_ref[i] = 0
        return carry

    def clear_slots(i, carry):
        table_ref[i] = 0
        live_ref[i] = 0
        tile_ref[i] = -1
        return carry

    lax.fori_loop(0, group, clear_used, 0)
    lax.fori_loop(0, group * cap, clear_slots, 0, unroll=8)

    def place(block, carry):
        owner = owner_ref[block]
        rank = used_ref[owner]
        used_ref[owner] = rank + 1
        where = owner * cap + rank
        table_ref[where] = block
        live_ref[where] = count_ref[block]
        tile_ref[where] = slot_ref[block]
        dest_ref[block] = where
        return carry

    lax.fori_loop(0, owner_ref.shape[0], place, 0)
    lane = lax.broadcasted_iota(jnp.int32, (1, LANES), 1)

    def mark(owner, carry):
        row = jnp.full((1, LANES), -1, jnp.int32)
        for i in range(cap):
            row = jnp.where(lane == i, tile_ref[owner * cap + i], row)
        marks_ref[owner] = row
        return carry

    lax.fori_loop(0, group, mark, 0)


def plan(cap, group, owner, slot, count):
    slots = group * cap
    return pl.pallas_call(
        functools.partial(plan_kernel, cap),
        name="plan",
        out_shape=(
            jax.ShapeDtypeStruct((slots,), jnp.int32),
            jax.ShapeDtypeStruct((slots,), jnp.int32),
            jax.ShapeDtypeStruct(owner.shape, jnp.int32),
            jax.ShapeDtypeStruct((group, 1, LANES), jnp.int32),
        ),
        in_specs=[SMEM] * 3,
        out_specs=(SMEM, SMEM, SMEM, VMEM),
        scratch_shapes=[pltpu.SMEM((group,), jnp.int32), pltpu.SMEM((slots,), jnp.int32)],
    )(owner, slot, count)


class Group:
    def __init__(self):
        self.wide = lax.axis_size(GROUP_AXES[1])
        self.size = lax.axis_size(GROUP_AXES)
        self.me = lax.axis_index(GROUP_AXES[0]) * self.wide + lax.axis_index(GROUP_AXES[1])

    def device(self, peer):
        return {GROUP_AXES[0]: peer // self.wide, GROUP_AXES[1]: peer % self.wide}

    def greet(self):
        barrier = pltpu.get_barrier_semaphore()

        def signal(k, carry):
            pl.semaphore_signal(
                barrier, inc=1, device_id=self.device(self.me ^ k), device_id_type=MESH
            )
            return carry

        lax.fori_loop(1, self.size, signal, 0)

    def gathered(self):
        pl.semaphore_wait(pltpu.get_barrier_semaphore(), self.size - 1)


def twice(rows):
    return jnp.concatenate([rows, rows], axis=0)


def span_of(part):
    return slice(part * LANES, (part + 1) * LANES)


def encode(code):
    power = code >> 8
    scale = jnp.where(
        power < 28,
        (1 << (power & 31)).astype(F32),
        (1 << jnp.maximum(power - 28, 0)).astype(F32) * 2.0**28,
    )
    size = ((code & 127) + 128).astype(F32) * (scale * 2.0**-28)
    return jnp.where((code & 128) != 0, -size, size)


def decode(value):
    size = jnp.abs(value)
    position = jnp.where(value < 0.0, 128.0 / QUANT, 0.0)
    for bit in (32, 16, 8, 4, 2, 1):
        large = size >= 2.0 ** (7 + bit - 28)
        size = jnp.where(large, size * 2.0**-bit, size)
        position = jnp.where(large, position + bit * 256.0 / QUANT, position)
    return position + (size * (2.0**28 / QUANT) + (0.5 + 0.5 / QUANT - 128.0 / QUANT))


def load_item(u, item_ref, fields_ref):
    rows = item_ref.shape[0]
    first = u * rows
    fields_ref[first : first + rows] = item_ref[...].astype(F32)
    for q in range(rows // FIELDS):
        base = first + q * FIELDS
        fields_ref[base + 13 : base + 16] = decode(fields_ref[base + 13 : base + 16])

    def spread(field, part):
        return twice(
            jnp.concatenate(
                [
                    jnp.broadcast_to(fields_ref[pl.ds(row, 1), :], (8, LANES))
                    for row in (
                        first + (part * 2) * FIELDS + field,
                        first + (part * 2 + 1) * FIELDS + field,
                    )
                ],
                axis=1,
            )
        )

    return spread


def stencil(position, node):
    offset = node - position
    magnitude = jnp.abs(offset)
    outer_part = jnp.maximum(1.5 - magnitude, 0.0)
    weight = jnp.where(
        magnitude < 0.5, 0.75 - magnitude * magnitude, 0.5 * outer_part * outer_part
    )
    return weight, weight * offset


def planes(u, spread, part, node, rows_ref):
    factors_y = stencil(spread(14, part), node)
    factors_z = [factor.astype(BF16) for factor in stencil(spread(15, part), node)]
    firsts = [((u * 2 + part) * 2 + k) * 2 * EDGE for k in range(2)]
    for first, factor in zip(firsts, factors_y):
        for q in range(2):
            rows_ref[first + q * EDGE : first + (q + 1) * EDGE] = factor[:, span_of(q)]

    def row(first, y):
        return jnp.concatenate(
            [
                twice(
                    jnp.broadcast_to(rows_ref[pl.ds(first + q * EDGE + y, 1), :], (8, LANES))
                ).astype(BF16)
                for q in range(2)
            ],
            axis=1,
        )

    zero, one, two = [], [], []
    for y in range(EDGE):
        weight_row, slope_row = row(firsts[0], y), row(firsts[1], y)
        zero.append(weight_row * factors_z[0])
        one.append(slope_row * factors_z[0])
        two.append(weight_row * factors_z[1])
    return [jnp.concatenate(parts, axis=0) for parts in (zero, one, two)]


def nodes():
    return lax.broadcasted_iota(jnp.int32, (EDGE, 2 * LANES), 0).astype(F32)


def deposit(u, item_ref, fields_ref, rows_ref):
    spread = load_item(u, item_ref, fields_ref)
    node = nodes()
    total = None
    for part in range(item_ref.shape[0] // (2 * FIELDS)):
        weight_x, slope_x = stencil(spread(13, part), node)
        mass = spread(0, part)
        mass_x = mass * weight_x
        mass_slope = mass * slope_x
        nothing = jnp.zeros(mass_x.shape, BF16)
        lead_zero, lead_one, lead_two = [mass_x.astype(BF16)], [nothing], [nothing]
        for d in range(3):
            lead_zero.append(
                (spread(1 + d, part) * mass_x + spread(4 + 3 * d, part) * mass_slope).astype(BF16)
            )
            lead_one.append((spread(5 + 3 * d, part) * mass_x).astype(BF16))
            lead_two.append((spread(6 + 3 * d, part) * mass_x).astype(BF16))
        lead = jnp.concatenate(
            [jnp.concatenate(rows, axis=0) for rows in (lead_zero, lead_one, lead_two)], axis=1
        )
        plane = jnp.concatenate(planes(u, spread, part, node, rows_ref), axis=1)
        sums = lax.dot_general(
            lead, plane, (((1,), (1,)), ((), ())), preferred_element_type=F32
        )
        total = sums if total is None else total + sums
    return total


def interpolate(u, item_ref, grid_rows, fields_ref, rows_ref, parts_ref):
    spread = load_item(u, item_ref, fields_ref)
    node = nodes()
    quarters = item_ref.shape[0] // FIELDS
    first = u * quarters * RESULTS * 8
    for part in range(quarters // 2):
        weight_x, slope_x = stencil(spread(13, part), node)
        moments = [
            jnp.dot(grid_rows, plane, preferred_element_type=F32)
            for plane in planes(u, spread, part, node, rows_ref)
        ]
        slope_four = 4.0 * slope_x
        weight_four = 4.0 * weight_x
        for d in range(3):
            span = slice(d * EDGE, (d + 1) * EDGE)
            entries = (
                (d, weight_x, moments[0]),
                (3 + 3 * d, slope_four, moments[0]),
                (4 + 3 * d, weight_four, moments[1]),
                (5 + 3 * d, weight_four, moments[2]),
            )
            for entry, factor, moment in entries:
                product = factor * moment[span]
                partial = product[:8] + product[8:]
                for q in range(2):
                    at = first + ((part * 2 + q) * RESULTS + entry) * 8
                    parts_ref[at : at + 8] = partial[:, span_of(q)]
    groups = []
    for g in range(quarters * RESULTS // 8):
        total = parts_ref[pl.ds(first + g * 64, 8, stride=8), :]
        for j in range(1, 8):
            total = total + parts_ref[pl.ds(first + g * 64 + j, 8, stride=8), :]
        groups.append(total)
    return jnp.concatenate(groups, axis=0).astype(BF16)


def scatter_kernel(
    cap,
    subs,
    table_ref,
    live_ref,
    marks_ref,
    mass_ref,
    velocity_ref,
    affine_ref,
    cell_ref,
    fraction_ref,
    arrived_ref,
    sums_ref,
    told_ref,
    mass_v,
    velocity_v,
    affine_v,
    cell_v,
    fraction_v,
    stage_ref,
    packed_ref,
    fields_ref,
    rows_ref,
    load_sems,
    send_sems,
    recv_sems,
    mark_send,
    mark_recv,
):
    group = Group()
    n, me = group.size, group.me
    per = cap // subs
    blocks, _, width = mass_v.shape
    quarters = width // LANES
    sources = (velocity_ref, affine_ref, cell_ref, fraction_ref)
    staged = (velocity_v, affine_v, cell_v, fraction_v)
    mass_load = pltpu.make_async_copy(mass_ref, mass_v, load_sems.at[len(sources)])
    mass_load.start()

    def load_block(block, carry):
        cols = pl.ds(pl.multiple_of(block * width, LANES), width)
        for i, (source, target) in enumerate(zip(sources, staged)):
            pltpu.make_async_copy(
                source.at[:, cols], target.at[block], load_sems.at[i]
            ).start()
        return carry

    lax.fori_loop(0, blocks, load_block, 0, unroll=4)
    group.greet()
    lane = lax.broadcasted_iota(jnp.int32, (1, width), 1)
    mass_load.wait()
    for i, target in enumerate(staged):
        pltpu.make_async_copy(target, target, load_sems.at[i]).wait()

    def pack(slot):
        block = table_ref[slot]
        live = jnp.where(lane < live_ref[slot], mass_v[block], 0.0)
        velocity = velocity_v[block]
        affine = affine_v[block]
        code = encode(cell_v[block] * QUANT + fraction_v[block])
        for q in range(quarters):
            base = q * FIELDS
            stage_ref[base : base + 1] = live[:, span_of(q)]
            stage_ref[base + 1 : base + 4] = velocity[:, span_of(q)]
            stage_ref[base + 4 : base + 13] = affine[:, span_of(q)]
            stage_ref[base + 13 : base + 16] = code[:, span_of(q)]
        packed_ref[slot] = stage_ref[...].astype(BF16)

    def rows_of(device, sub):
        return pl.ds(device * cap + sub * per, per)

    def transfer(k, sub):
        peer = me ^ k
        return pltpu.make_async_remote_copy(
            src_ref=packed_ref.at[rows_of(peer, sub)],
            dst_ref=arrived_ref.at[rows_of(me, sub)],
            send_sem=send_sems.at[k, sub],
            recv_sem=recv_sems.at[k, sub],
            device_id=group.device(peer),
            device_id_type=MESH,
        )

    def arrival(k, sub):
        rows = rows_of(me ^ k, sub)
        return pltpu.make_async_copy(
            packed_ref.at[rows], arrived_ref.at[rows], recv_sems.at[k, sub]
        )

    def mark_transfer(k):
        peer = me ^ k
        return pltpu.make_async_remote_copy(
            src_ref=marks_ref.at[peer],
            dst_ref=told_ref.at[me],
            send_sem=mark_send.at[k],
            recv_sem=mark_recv.at[k],
            device_id=group.device(peer),
            device_id_type=MESH,
        )

    own_marks = pltpu.make_async_copy(marks_ref.at[me], told_ref.at[me], mark_recv.at[0])
    own_marks.start()

    def pack_step(step):
        k = n - 1 - step % n
        sub = step // n
        for i in range(per):
            pack((me ^ k) * cap + sub * per + i)

    def send_step(step):
        k = n - 1 - step % n
        sub = step // n

        @pl.when(k != 0)
        def _():
            transfer(k, sub).start()

        @pl.when(k == 0)
        def _():
            arrival(0, sub).start()

    pack_step(0)
    group.gathered()

    def pack_and_send(step, carry):
        pack_step(step)
        send_step(step - 1)
        return carry

    lax.fori_loop(1, n * subs, pack_and_send, 0)

    def send_marks(k, carry):
        mark_transfer(k).start()
        return carry

    lax.fori_loop(1, n, send_marks, 0)
    send_step(n * subs - 1)

    pair = 2

    def take(step, carry):
        sub = step // (n // pair)
        first = (step % (n // pair)) * pair
        for j in range(pair):
            arrival(first + j, sub).wait()
        for j in range(pair):
            for i in range(per):
                slot = (me ^ (first + j)) * cap + sub * per + i
                sums_ref[slot] = deposit(
                    j * per + i, arrived_ref.at[slot], fields_ref, rows_ref
                )
        return carry

    lax.fori_loop(0, n // pair * subs, take, 0)
    own_marks.wait()

    def settle(k, carry):
        mark_transfer(k).wait_recv()
        mark_transfer(k).wait_send()
        for sub in range(subs):
            transfer(k, sub).wait_send()
        return carry

    lax.fori_loop(1, n, settle, 0)


def scatter(cap, subs, group, table, live, marks, mass, velocity, affine, cell, fraction):
    slots = group * cap
    blocks, _, width = mass.shape
    quarters = width // LANES
    rows = quarters * FIELDS
    unroll = 2 * (cap // subs)
    arrays = (mass, velocity, affine, cell, fraction)
    return pl.pallas_call(
        functools.partial(scatter_kernel, cap, subs),
        name="scatter_step",
        out_shape=(
            jax.ShapeDtypeStruct((slots, rows, LANES), BF16),
            jax.ShapeDtypeStruct((slots, 4 * EDGE, EDGE * EDGE), F32),
            jax.ShapeDtypeStruct(marks.shape, jnp.int32),
        ),
        in_specs=[SMEM, SMEM, VMEM] + [HBM] * 5,
        out_specs=(VMEM,) * 3,
        scratch_shapes=[pltpu.VMEM(mass.shape, F32)]
        + [
            pltpu.VMEM((blocks, array.shape[0], width), array.dtype) for array in arrays[1:]
        ]
        + [
            pltpu.VMEM((rows, LANES), F32),
            pltpu.VMEM((slots, rows, LANES), BF16),
            pltpu.VMEM((unroll * rows, LANES), F32),
            pltpu.VMEM((unroll * 2 * quarters * EDGE, LANES), F32),
            pltpu.SemaphoreType.DMA((len(arrays),)),
            pltpu.SemaphoreType.DMA((group, subs)),
            pltpu.SemaphoreType.DMA((group, subs)),
            pltpu.SemaphoreType.DMA((group,)),
            pltpu.SemaphoreType.DMA((group,)),
        ],
        compiler_params=pltpu.CompilerParams(
            collective_id=0, has_side_effects=True, vmem_limit_bytes=40 << 20
        ),
        cost_estimate=cost(10**10),
    )(table, live, marks, *arrays)


def grid_kernel(cap, told_ref, deposits_ref, drag_ref, grid_ref, round_ref, sums_ref):
    plane_size = EDGE * EDGE

    def start(t, carry):
        for x in range(EDGE):
            sums_ref[t, x : x + 1, :] = drag_ref[
                pl.ds(t, 1), x * plane_size : (x + 1) * plane_size
            ]
        sums_ref[t, EDGE:, :] = jnp.zeros((3 * EDGE, plane_size), F32)
        return carry

    lax.fori_loop(0, drag_ref.shape[0], start, 0)

    def add(device, carry):
        for i in range(cap):
            tile = told_ref[device, 0, i]

            @pl.when(tile >= 0)
            def _():
                sums_ref[tile] += deposits_ref[device * cap + i]

        return carry

    lax.fori_loop(0, told_ref.shape[0], add, 0)

    def divide(t, carry):
        mass = sums_ref[t, :EDGE, :]
        parts = [sums_ref[t, (d + 1) * EDGE : (d + 2) * EDGE, :] / mass for d in range(3)]
        round_ref[t] = jnp.concatenate(parts, axis=0).astype(BF16)
        for d in range(3):
            for x in range(EDGE):
                grid_ref[d, pl.ds(t, 1), x * plane_size : (x + 1) * plane_size] = parts[d][
                    x : x + 1
                ]
        return carry

    lax.fori_loop(0, round_ref.shape[0], divide, 0)


def grid_step(cap, told, deposits, drag):
    tiles = drag.shape[0]
    plane_size = EDGE * EDGE
    return pl.pallas_call(
        functools.partial(grid_kernel, cap),
        name="grid_step",
        out_shape=(
            jax.ShapeDtypeStruct((3, tiles, EDGE * plane_size), F32),
            jax.ShapeDtypeStruct((tiles, 3 * EDGE, plane_size), BF16),
        ),
        in_specs=[SMEM, VMEM, VMEM],
        out_specs=(VMEM, VMEM),
        scratch_shapes=[pltpu.VMEM((tiles, 4 * EDGE, plane_size), F32)],
        compiler_params=pltpu.CompilerParams(vmem_limit_bytes=20 << 20),
        cost_estimate=cost(10**9),
    )(told, deposits, drag)


def gather_kernel(
    cap,
    subs,
    told_ref,
    arrived_ref,
    round_ref,
    returned_ref,
    results_ref,
    fields_ref,
    rows_ref,
    parts_ref,
    send_sems,
    recv_sems,
):
    group = Group()
    n, me = group.size, group.me
    per = cap // subs
    group.greet()

    def rows_of(device, sub):
        return pl.ds(device * cap + sub * per, per)

    def transfer(k, sub):
        peer = me ^ k
        return pltpu.make_async_remote_copy(
            src_ref=results_ref.at[rows_of(peer, sub)],
            dst_ref=returned_ref.at[rows_of(me, sub)],
            send_sem=send_sems.at[k, sub],
            recv_sem=recv_sems.at[k, sub],
            device_id=group.device(peer),
            device_id_type=MESH,
        )

    def arrival(k, sub):
        rows = rows_of(me ^ k, sub)
        return pltpu.make_async_copy(
            results_ref.at[rows], returned_ref.at[rows], recv_sems.at[k, sub]
        )

    pair = 2
    half = n // 2
    strides = half // pair

    def place(step):
        side = step // (strides * subs)
        rest = step % (strides * subs)
        return n - 1 - side * half - (rest % strides) * pair, rest // strides

    def work(step):
        top, sub = place(step)
        for j in range(pair):
            source = me ^ (top - j)
            for i in range(per):
                slot = source * cap + sub * per + i
                tile = jnp.maximum(told_ref[source, 0, sub * per + i], 0)
                results_ref[slot] = interpolate(
                    j * per + i,
                    arrived_ref.at[slot],
                    round_ref[tile],
                    fields_ref,
                    rows_ref,
                    parts_ref,
                )

    def send(step):
        top, sub = place(step)
        for j in range(pair):
            k = top - j

            @pl.when(k != 0)
            def _():
                transfer(k, sub).start()

            @pl.when(k == 0)
            def _():
                arrival(0, sub).start()

    steps = half // pair * subs * 2
    work(0)
    group.gathered()

    def work_and_send(step, carry):
        work(step)
        send(step - 1)
        return carry

    lax.fori_loop(1, steps, work_and_send, 0)
    send(steps - 1)

    def settle(k, carry):
        for sub in range(subs):
            transfer(k, sub).wait_recv()
            transfer(k, sub).wait_send()
        return carry

    for sub in range(subs):
        arrival(0, sub).wait()
    lax.fori_loop(1, n, settle, 0)


def gather(cap, subs, told, arrived, rounded):
    slots, rows, _ = arrived.shape
    group = told.shape[0]
    quarters = rows // FIELDS
    unroll = 2 * (cap // subs)
    result = (slots, quarters * RESULTS, LANES)
    return pl.pallas_call(
        functools.partial(gather_kernel, cap, subs),
        name="gather_step",
        out_shape=jax.ShapeDtypeStruct(result, BF16),
        in_specs=[SMEM, VMEM, VMEM],
        out_specs=VMEM,
        scratch_shapes=[
            pltpu.VMEM(result, BF16),
            pltpu.VMEM((unroll * rows, LANES), F32),
            pltpu.VMEM((unroll * 2 * quarters * EDGE, LANES), F32),
            pltpu.VMEM((unroll * quarters * RESULTS * 8, LANES), F32),
            pltpu.SemaphoreType.DMA((group, subs)),
            pltpu.SemaphoreType.DMA((group, subs)),
        ],
        compiler_params=pltpu.CompilerParams(
            collective_id=1, has_side_effects=True, vmem_limit_bytes=40 << 20
        ),
        cost_estimate=cost(10**10),
    )(told, arrived, rounded)


def unpack_kernel(dest_ref, count_ref, returned_ref, velocity_ref, affine_ref):
    blocks = dest_ref.shape[0]
    width = velocity_ref.shape[1] // blocks
    lane = lax.broadcasted_iota(jnp.int32, (1, LANES), 1)

    def unpack(block, carry):
        count = count_ref[block]
        rows = returned_ref[dest_ref[block]].astype(F32)
        for q in range(width // LANES):
            first = q * LANES
            cols = pl.ds(pl.multiple_of(block * width + first, LANES), LANES)
            part = jnp.where(lane + first < count, rows[q * RESULTS : (q + 1) * RESULTS], 0.0)
            velocity_ref[:, cols] = part[:3]
            affine_ref[:, cols] = part[3:]
        return carry

    lax.fori_loop(0, blocks, unpack, 0)


def unpack(dest, count, returned, width):
    particles = dest.shape[0] * width
    return pl.pallas_call(
        unpack_kernel,
        name="unpack",
        out_shape=(
            jax.ShapeDtypeStruct((3, particles), F32),
            jax.ShapeDtypeStruct((9, particles), F32),
        ),
        in_specs=[SMEM, SMEM, VMEM],
        out_specs=(VMEM, VMEM),
        compiler_params=pltpu.CompilerParams(vmem_limit_bytes=20 << 20),
    )(dest, count, returned)


def per_device(
    particle_mass,
    particle_velocity,
    particle_affine,
    particle_cell,
    particle_fraction,
    block_owner,
    block_slot,
    block_count,
    cell_drag,
):
    group = lax.axis_size(GROUP_AXES)
    blocks = block_count.shape[0]
    width = particle_mass.shape[0] // blocks
    cap = max(1, 2 * blocks // group)
    subs = min(cap, PARTS)
    table, live, dest, marks = plan(cap, group, block_owner[:, 0], block_slot, block_count)
    arrived, deposits, told = scatter(
        cap,
        subs,
        group,
        table,
        live,
        marks,
        particle_mass.reshape(blocks, 1, width),
        particle_velocity,
        particle_affine,
        particle_cell,
        particle_fraction,
    )
    grid_velocity, rounded = grid_step(cap, told, deposits, cell_drag)
    returned = gather(cap, subs, told, arrived, rounded)
    new_velocity, new_affine = unpack(dest, block_count, returned, width)
    return jnp.transpose(grid_velocity, (1, 0, 2)), new_velocity, new_affine


def solution(mesh):
    everywhere = ("gx", "gy", "gz")
    return jax.shard_map(
        per_device,
        mesh=mesh,
        in_specs=(
            P(everywhere),
            P(None, everywhere),
            P(None, everywhere),
            P(None, everywhere),
            P(None, everywhere),
            P(everywhere, None),
            P(everywhere),
            P(everywhere),
            P(everywhere, None),
        ),
        out_specs=(P(everywhere, None, None), P(None, everywhere), P(None, everywhere)),
        check_vma=False,
    )
```

```python
import functools

import jax
import jax.numpy as jnp
from jax import lax
from jax.experimental import pallas as pl
from jax.experimental.pallas import tpu as pltpu
from jax.sharding import PartitionSpec as P

EDGE = 16
QUANT = 1024
LANES = 128
FIELDS = 16
RESULTS = 12
PARTS = 4
UNROLL = 4
GROUP_AXES = ("gy", "gz")
F32 = jnp.float32
BF16 = jnp.bfloat16
MESH = pl.DeviceIdType.MESH


SMEM = pl.BlockSpec(memory_space=pltpu.SMEM)
VMEM = pl.BlockSpec(memory_space=pltpu.VMEM)
HBM = pl.BlockSpec(memory_space=pltpu.HBM)


def cost(flops):
    return pl.CostEstimate(flops=flops, bytes_accessed=1 << 22, transcendentals=0)


def twice(rows):
    return jnp.concatenate([rows, rows], axis=0)


def span_of(part):
    return slice(part * LANES, (part + 1) * LANES)


def encode(code):
    power = code >> 8
    scale = jnp.where(
        power < 28,
        (1 << (power & 31)).astype(F32),
        (1 << jnp.maximum(power - 28, 0)).astype(F32) * 2.0**28,
    )
    size = ((code & 127) + 128).astype(F32) * (scale * 2.0**-28)
    return jnp.where((code & 128) != 0, -size, size)


def pack_kernel(
    cap,
    owner_ref,
    slot_ref,
    count_ref,
    mass_ref,
    velocity_ref,
    affine_ref,
    cell_ref,
    fraction_ref,
    packed_ref,
    dest_ref,
    marks_ref,
    used_ref,
    tile_ref,
    stage_ref,
    mass_v,
    velocity_v,
    affine_v,
    cell_v,
    fraction_v,
    load_sems,
):
    sources = (mass_ref, velocity_ref, affine_ref, cell_ref, fraction_ref)
    staged = (mass_v, velocity_v, affine_v, cell_v, fraction_v)
    loads = [
        pltpu.make_async_copy(source, target, load_sems.at[i])
        for i, (source, target) in enumerate(zip(sources, staged))
    ]
    for load in loads:
        load.start()
    group = used_ref.shape[0]
    blocks, _, width = mass_v.shape
    quarters = width // LANES
    rows = quarters * FIELDS

    def clear_used(i, carry):
        used_ref[i] = 0
        return carry

    def clear_slots(i, carry):
        tile_ref[i] = -1
        packed_ref[i] = jnp.zeros((rows, LANES), BF16)
        return carry

    lax.fori_loop(0, group, clear_used, 0, unroll=8)
    lax.fori_loop(0, group * cap, clear_slots, 0, unroll=8)

    def place(block, carry):
        owner = owner_ref[block]
        rank = used_ref[owner]
        used_ref[owner] = rank + 1
        where = owner * cap + rank
        tile_ref[where] = slot_ref[block]
        dest_ref[block] = where
        return carry

    lax.fori_loop(0, blocks, place, 0, unroll=2)
    lane = lax.broadcasted_iota(jnp.int32, (1, LANES), 1)

    def mark(owner, carry):
        row = jnp.full((1, LANES), -1, jnp.int32)
        for i in range(cap):
            row = jnp.where(lane == i, tile_ref[owner * cap + i], row)
        marks_ref[owner] = row
        return carry

    lax.fori_loop(0, group, mark, 0, unroll=2)
    for load in loads:
        load.wait()
    place_lane = lax.broadcasted_iota(jnp.int32, (1, width), 1)

    def pack(step, carry):
        for u in range(UNROLL):
            block = step * UNROLL + u
            cols = pl.ds(pl.multiple_of(block * width, LANES), width)
            live = jnp.where(place_lane < count_ref[block], mass_v[block], 0.0)
            velocity = velocity_v[:, cols]
            affine = affine_v[:, cols]
            code = encode(cell_v[:, cols] * QUANT + fraction_v[:, cols])
            for q in range(quarters):
                base = u * rows + q * FIELDS
                stage_ref[base : base + 1] = live[:, span_of(q)]
                stage_ref[base + 1 : base + 4] = velocity[:, span_of(q)]
                stage_ref[base + 4 : base + 13] = affine[:, span_of(q)]
                stage_ref[base + 13 : base + 16] = code[:, span_of(q)]
        for u in range(UNROLL):
            packed_ref[dest_ref[step * UNROLL + u]] = stage_ref[
                u * rows : (u + 1) * rows
            ].astype(BF16)
        return carry

    lax.fori_loop(0, blocks // UNROLL, pack, 0)


def pack(cap, group, owner, slot, count, mass, velocity, affine, cell, fraction):
    slots = group * cap
    blocks, _, width = mass.shape
    rows = width // LANES * FIELDS
    arrays = (mass, velocity, affine, cell, fraction)
    return pl.pallas_call(
        functools.partial(pack_kernel, cap),
        name="pack",
        out_shape=(
            pltpu.VMEM((slots, rows, LANES), BF16),
            jax.ShapeDtypeStruct(owner.shape, jnp.int32),
            pltpu.VMEM((group, 1, LANES), jnp.int32),
        ),
        in_specs=[SMEM] * 3 + [HBM] * 5,
        out_specs=(VMEM, SMEM, VMEM),
        scratch_shapes=[
            pltpu.SMEM((group,), jnp.int32),
            pltpu.SMEM((slots,), jnp.int32),
            pltpu.VMEM((UNROLL * rows, LANES), F32),
        ]
        + [pltpu.VMEM(array.shape, array.dtype) for array in arrays]
        + [pltpu.SemaphoreType.DMA((len(arrays),))],
        compiler_params=pltpu.CompilerParams(vmem_limit_bytes=60 << 20),
    )(owner, slot, count, *arrays)


def pieces(subs):
    return [(0, 1), (1, 1), (2, 2)] if subs == 4 else [(sub, 1) for sub in range(subs)]


class Group:
    def __init__(self):
        self.wide = lax.axis_size(GROUP_AXES[1])
        self.size = lax.axis_size(GROUP_AXES)
        self.me = lax.axis_index(GROUP_AXES[0]) * self.wide + lax.axis_index(GROUP_AXES[1])

    def device(self, peer):
        return {GROUP_AXES[0]: peer // self.wide, GROUP_AXES[1]: peer % self.wide}

    def greet(self):
        barrier = pltpu.get_barrier_semaphore()

        def signal(k, carry):
            pl.semaphore_signal(
                barrier, inc=1, device_id=self.device(self.me ^ k), device_id_type=MESH
            )
            return carry

        lax.fori_loop(1, self.size, signal, 0)

    def gathered(self):
        pl.semaphore_wait(pltpu.get_barrier_semaphore(), self.size - 1)


def decode(value):
    size = jnp.abs(value)
    position = jnp.where(value < 0.0, 128.0 / QUANT, 0.0)
    for bit in (32, 16, 8, 4, 2, 1):
        large = size >= 2.0 ** (7 + bit - 28)
        size = jnp.where(large, size * 2.0**-bit, size)
        position = jnp.where(large, position + bit * 256.0 / QUANT, position)
    return position + (size * (2.0**28 / QUANT) + (0.5 + 0.5 / QUANT - 128.0 / QUANT))


def load_item(u, item_ref, fields_ref):
    rows = item_ref.shape[0]
    first = u * rows
    fields_ref[first : first + rows] = item_ref[...].astype(F32)
    for q in range(rows // FIELDS):
        base = first + q * FIELDS
        fields_ref[base + 13 : base + 16] = decode(fields_ref[base + 13 : base + 16])

    def spread(field, part):
        return twice(
            jnp.concatenate(
                [
                    jnp.broadcast_to(fields_ref[pl.ds(row, 1), :], (8, LANES))
                    for row in (
                        first + (part * 2) * FIELDS + field,
                        first + (part * 2 + 1) * FIELDS + field,
                    )
                ],
                axis=1,
            )
        )

    return spread


def stencil(position, node):
    offset = node - position
    magnitude = jnp.abs(offset)
    outer_part = jnp.maximum(1.5 - magnitude, 0.0)
    weight = jnp.where(
        magnitude < 0.5, 0.75 - magnitude * magnitude, 0.5 * outer_part * outer_part
    )
    return weight, weight * offset


def planes(u, spread, part, node, rows_ref):
    factors_y = stencil(spread(14, part), node)
    factors_z = [factor.astype(BF16) for factor in stencil(spread(15, part), node)]
    firsts = [((u * 2 + part) * 2 + k) * 2 * EDGE for k in range(2)]
    for first, factor in zip(firsts, factors_y):
        for q in range(2):
            rows_ref[first + q * EDGE : first + (q + 1) * EDGE] = factor[:, span_of(q)]

    def row(first, y):
        return jnp.concatenate(
            [
                twice(
                    jnp.broadcast_to(rows_ref[pl.ds(first + q * EDGE + y, 1), :], (8, LANES))
                ).astype(BF16)
                for q in range(2)
            ],
            axis=1,
        )

    zero, one, two = [], [], []
    for y in range(EDGE):
        weight_row, slope_row = row(firsts[0], y), row(firsts[1], y)
        zero.append(weight_row * factors_z[0])
        one.append(slope_row * factors_z[0])
        two.append(weight_row * factors_z[1])
    return [jnp.concatenate(parts, axis=0) for parts in (zero, one, two)]


def nodes():
    return lax.broadcasted_iota(jnp.int32, (EDGE, 2 * LANES), 0).astype(F32)


def deposit(u, item_ref, fields_ref, rows_ref):
    spread = load_item(u, item_ref, fields_ref)
    node = nodes()
    total = None
    for part in range(item_ref.shape[0] // (2 * FIELDS)):
        weight_x, slope_x = stencil(spread(13, part), node)
        mass = spread(0, part)
        mass_x = mass * weight_x
        mass_slope = mass * slope_x
        nothing = jnp.zeros(mass_x.shape, BF16)
        lead_zero, lead_one, lead_two = [mass_x.astype(BF16)], [nothing], [nothing]
        for d in range(3):
            lead_zero.append(
                (spread(1 + d, part) * mass_x + spread(4 + 3 * d, part) * mass_slope).astype(BF16)
            )
            lead_one.append((spread(5 + 3 * d, part) * mass_x).astype(BF16))
            lead_two.append((spread(6 + 3 * d, part) * mass_x).astype(BF16))
        lead = jnp.concatenate(
            [jnp.concatenate(rows, axis=0) for rows in (lead_zero, lead_one, lead_two)], axis=1
        )
        plane = jnp.concatenate(planes(u, spread, part, node, rows_ref), axis=1)
        sums = lax.dot_general(
            lead, plane, (((1,), (1,)), ((), ())), preferred_element_type=F32
        )
        total = sums if total is None else total + sums
    return total


def interpolate(u, item_ref, grid_rows, fields_ref, rows_ref, parts_ref):
    spread = load_item(u, item_ref, fields_ref)
    node = nodes()
    quarters = item_ref.shape[0] // FIELDS
    first = u * quarters * RESULTS * 8
    for part in range(quarters // 2):
        weight_x, slope_x = stencil(spread(13, part), node)
        moments = [
            jnp.dot(grid_rows, plane, preferred_element_type=F32)
            for plane in planes(u, spread, part, node, rows_ref)
        ]
        slope_four = 4.0 * slope_x
        weight_four = 4.0 * weight_x
        for d in range(3):
            span = slice(d * EDGE, (d + 1) * EDGE)
            entries = (
                (d, weight_x, moments[0]),
                (3 + 3 * d, slope_four, moments[0]),
                (4 + 3 * d, weight_four, moments[1]),
                (5 + 3 * d, weight_four, moments[2]),
            )
            for entry, factor, moment in entries:
                product = factor * moment[span]
                partial = product[:8] + product[8:]
                for q in range(2):
                    at = first + ((part * 2 + q) * RESULTS + entry) * 8
                    parts_ref[at : at + 8] = partial[:, span_of(q)]
    groups = []
    for g in range(quarters * RESULTS // 8):
        total = parts_ref[pl.ds(first + g * 64, 8, stride=8), :]
        for j in range(1, 8):
            total = total + parts_ref[pl.ds(first + g * 64 + j, 8, stride=8), :]
        groups.append(total)
    return jnp.concatenate(groups, axis=0).astype(BF16)


def scatter_kernel(
    cap,
    subs,
    packed_ref,
    marks_ref,
    arrived_ref,
    sums_ref,
    told_ref,
    fields_ref,
    rows_ref,
    send_sems,
    recv_sems,
    mark_send,
    mark_recv,
):
    group = Group()
    n, me = group.size, group.me
    per = cap // subs
    group.greet()

    def rows_of(device, sub):
        return pl.ds(device * cap + sub * per, per)

    def transfer(k, sub):
        peer = me ^ k
        return pltpu.make_async_remote_copy(
            src_ref=packed_ref.at[rows_of(peer, sub)],
            dst_ref=arrived_ref.at[rows_of(me, sub)],
            send_sem=send_sems.at[k, sub],
            recv_sem=recv_sems.at[k, sub],
            device_id=group.device(peer),
            device_id_type=MESH,
        )

    def arrival(k, sub):
        rows = rows_of(me ^ k, sub)
        return pltpu.make_async_copy(
            packed_ref.at[rows], arrived_ref.at[rows], recv_sems.at[k, sub]
        )

    def mark_transfer(k):
        peer = me ^ k
        return pltpu.make_async_remote_copy(
            src_ref=marks_ref.at[peer],
            dst_ref=told_ref.at[me],
            send_sem=mark_send.at[k],
            recv_sem=mark_recv.at[k],
            device_id=group.device(peer),
            device_id_type=MESH,
        )

    own_marks = pltpu.make_async_copy(marks_ref.at[me], told_ref.at[me], mark_recv.at[0])
    own_marks.start()

    for sub in range(subs):
        arrival(0, sub).start()
    group.gathered()
    half = n // 2

    def send_near(step, carry):
        transfer(1 + step // subs, step % subs).start()
        return carry

    def send_far(step, carry):
        transfer(half + step % half, step // half).start()
        return carry

    def send_marks(k, carry):
        mark_transfer(k).start()
        return carry

    lax.fori_loop(0, (half - 1) * subs, send_near, 0)
    lax.fori_loop(0, half * subs, send_far, 0)
    lax.fori_loop(1, n, send_marks, 0)
    pair = 2
    strides = half // pair

    def take(step, carry):
        side = step // (strides * subs)
        rest = step % (strides * subs)
        sub = (1 - side) * (rest % subs) + side * (rest // strides)
        first = side * half + pair * ((1 - side) * (rest // subs) + side * (rest % strides))
        for j in range(pair):
            arrival(first + j, sub).wait()
        for j in range(pair):
            for i in range(per):
                slot = (me ^ (first + j)) * cap + sub * per + i
                sums_ref[slot] = deposit(
                    j * per + i, arrived_ref.at[slot], fields_ref, rows_ref
                )
        return carry

    lax.fori_loop(0, strides * subs * 2, take, 0)
    own_marks.wait()

    def settle(k, carry):
        mark_transfer(k).wait_recv()
        mark_transfer(k).wait_send()
        for sub in range(subs):
            transfer(k, sub).wait_send()
        return carry

    lax.fori_loop(1, n, settle, 0)


def scatter(cap, subs, packed, marks):
    slots, rows, _ = packed.shape
    group = marks.shape[0]
    quarters = rows // FIELDS
    unroll = 2 * (cap // subs)
    return pl.pallas_call(
        functools.partial(scatter_kernel, cap, subs),
        name="scatter_step",
        out_shape=(
            jax.ShapeDtypeStruct(packed.shape, BF16),
            jax.ShapeDtypeStruct((slots, 4 * EDGE, EDGE * EDGE), F32),
            jax.ShapeDtypeStruct(marks.shape, jnp.int32),
        ),
        in_specs=[VMEM, VMEM],
        out_specs=(VMEM,) * 3,
        scratch_shapes=[
            pltpu.VMEM((unroll * rows, LANES), F32),
            pltpu.VMEM((unroll * 2 * quarters * EDGE, LANES), F32),
            pltpu.SemaphoreType.DMA((group, subs)),
            pltpu.SemaphoreType.DMA((group, subs)),
            pltpu.SemaphoreType.DMA((group,)),
            pltpu.SemaphoreType.DMA((group,)),
        ],
        compiler_params=pltpu.CompilerParams(
            collective_id=0, has_side_effects=True, vmem_limit_bytes=30 << 20
        ),
        cost_estimate=cost(10**10),
    )(packed, marks)


def grid_kernel(cap, told_ref, deposits_ref, drag_ref, ratio_ref, round_ref, sums_ref):
    plane_size = EDGE * EDGE
    tiles = drag_ref.shape[0]

    def start(t, carry):
        for x in range(EDGE):
            sums_ref[t, x : x + 1, :] = drag_ref[
                pl.ds(t, 1), x * plane_size : (x + 1) * plane_size
            ]
        sums_ref[t, EDGE:, :] = jnp.zeros((3 * EDGE, plane_size), F32)
        return carry

    lax.fori_loop(0, tiles, start, 0, unroll=2)
    sums_ref[tiles] = jnp.zeros((4 * EDGE, plane_size), F32)

    def add(device, carry):
        for i in range(cap):
            mark = told_ref[device, 0, i]
            tile = jnp.where(mark < 0, tiles, mark)
            sums_ref[tile] += deposits_ref[device * cap + i]
        return carry

    lax.fori_loop(0, told_ref.shape[0], add, 0)

    def divide(t, carry):
        mass = sums_ref[t, :EDGE, :]
        ratio = jnp.concatenate(
            [sums_ref[t, (d + 1) * EDGE : (d + 2) * EDGE, :] / mass for d in range(3)], axis=0
        )
        ratio_ref[t] = ratio
        round_ref[t] = ratio.astype(BF16)
        return carry

    lax.fori_loop(0, tiles, divide, 0, unroll=2)


def grid_step(cap, told, deposits, drag):
    tiles = drag.shape[0]
    plane_size = EDGE * EDGE
    return pl.pallas_call(
        functools.partial(grid_kernel, cap),
        name="grid_step",
        out_shape=(
            pltpu.VMEM((tiles, 3 * EDGE, plane_size), F32),
            pltpu.VMEM((tiles, 3 * EDGE, plane_size), BF16),
        ),
        in_specs=[SMEM, VMEM, VMEM],
        out_specs=(VMEM, VMEM),
        scratch_shapes=[pltpu.VMEM((tiles + 1, 4 * EDGE, plane_size), F32)],
        compiler_params=pltpu.CompilerParams(vmem_limit_bytes=20 << 20),
        cost_estimate=cost(10**9),
    )(told, deposits, drag)


def gather_kernel(
    cap,
    subs,
    told_ref,
    arrived_ref,
    round_ref,
    ratio_ref,
    returned_ref,
    grid_ref,
    results_ref,
    fields_ref,
    rows_ref,
    parts_ref,
    send_sems,
    recv_sems,
):
    group = Group()
    n, me = group.size, group.me
    per = cap // subs
    group.greet()
    cuts = pieces(subs)

    def rows_of(device, piece):
        first, length = cuts[piece]
        return pl.ds(device * cap + first * per, length * per)

    def transfer(k, piece):
        peer = me ^ k
        return pltpu.make_async_remote_copy(
            src_ref=results_ref.at[rows_of(peer, piece)],
            dst_ref=returned_ref.at[rows_of(me, piece)],
            send_sem=send_sems.at[k, piece],
            recv_sem=recv_sems.at[k, piece],
            device_id=group.device(peer),
            device_id_type=MESH,
        )

    def arrival(k, piece):
        rows = rows_of(me ^ k, piece)
        return pltpu.make_async_copy(
            results_ref.at[rows], returned_ref.at[rows], recv_sems.at[k, piece]
        )

    pair = 2
    half = n // 2
    strides = half // pair

    def place(step):
        side = step // (strides * subs)
        rest = step % (strides * subs)
        return n - 1 - side * half - (rest % strides) * pair, rest // strides

    def work(step):
        top, sub = place(step)
        for j in range(pair):
            source = me ^ (top - j)
            for i in range(per):
                slot = source * cap + sub * per + i
                tile = jnp.maximum(told_ref[source, 0, sub * per + i], 0)
                results_ref[slot] = interpolate(
                    j * per + i,
                    arrived_ref.at[slot],
                    round_ref[tile],
                    fields_ref,
                    rows_ref,
                    parts_ref,
                )

    def send(step):
        top, sub = place(step)
        for piece, (first, length) in enumerate(cuts):
            for j in range(pair):
                k = top - j

                @pl.when((sub == first + length - 1) & (k != 0))
                def _():
                    transfer(k, piece).start()

                @pl.when((sub == first + length - 1) & (k == 0))
                def _():
                    arrival(0, piece).start()

    steps = half // pair * subs * 2
    work(0)
    group.gathered()

    def work_and_send(step, carry):
        work(step)
        send(step - 1)
        return carry

    lax.fori_loop(1, steps, work_and_send, 0)
    send(steps - 1)

    plane_size = EDGE * EDGE

    def spread_rows(t, carry):
        for d in range(3):
            for x in range(EDGE):
                row = d * EDGE + x
                grid_ref[d, pl.ds(t, 1), x * plane_size : (x + 1) * plane_size] = ratio_ref[
                    t, row : row + 1, :
                ]
        return carry

    lax.fori_loop(0, ratio_ref.shape[0], spread_rows, 0)

    def settle(k, carry):
        for piece in range(len(cuts)):
            transfer(k, piece).wait_recv()
            transfer(k, piece).wait_send()
        return carry

    for piece in range(len(cuts)):
        arrival(0, piece).wait()
    lax.fori_loop(1, n, settle, 0)


def gather(cap, subs, told, arrived, rounded, ratio):
    slots, rows, _ = arrived.shape
    group = told.shape[0]
    quarters = rows // FIELDS
    unroll = 2 * (cap // subs)
    result = (slots, quarters * RESULTS, LANES)
    return pl.pallas_call(
        functools.partial(gather_kernel, cap, subs),
        name="gather_step",
        out_shape=(
            pltpu.VMEM(result, BF16),
            pltpu.VMEM((3, ratio.shape[0], EDGE**3), F32),
        ),
        in_specs=[SMEM, VMEM, VMEM, VMEM],
        out_specs=(VMEM, VMEM),
        scratch_shapes=[
            pltpu.VMEM(result, BF16),
            pltpu.VMEM((unroll * rows, LANES), F32),
            pltpu.VMEM((unroll * 2 * quarters * EDGE, LANES), F32),
            pltpu.VMEM((unroll * quarters * RESULTS * 8, LANES), F32),
            pltpu.SemaphoreType.DMA((group, subs)),
            pltpu.SemaphoreType.DMA((group, subs)),
        ],
        compiler_params=pltpu.CompilerParams(
            collective_id=1, has_side_effects=True, vmem_limit_bytes=40 << 20
        ),
        cost_estimate=cost(10**10),
    )(told, arrived, rounded, ratio)


def unpack_kernel(
    dest_ref,
    count_ref,
    returned_ref,
    grid_ref,
    velocity_out,
    affine_out,
    grid_out,
    velocity_ref,
    affine_ref,
    sems,
):
    copies = [pltpu.make_async_copy(grid_ref, grid_out, sems.at[0, 0])]
    copies[0].start()
    blocks = dest_ref.shape[0]
    width = velocity_ref.shape[1] // blocks
    lane = lax.broadcasted_iota(jnp.int32, (1, LANES), 1)

    def unpack(block, carry):
        count = count_ref[block]
        rows = returned_ref[dest_ref[block]].astype(F32)
        for q in range(width // LANES):
            first = q * LANES
            cols = pl.ds(pl.multiple_of(block * width + first, LANES), LANES)
            part = jnp.where(lane + first < count, rows[q * RESULTS : (q + 1) * RESULTS], 0.0)
            velocity_ref[:, cols] = part[:3]
            affine_ref[:, cols] = part[3:]
        return carry

    share = blocks // PARTS
    for c in range(PARTS):
        lax.fori_loop(c * share, (c + 1) * share, unpack, 0, unroll=4)
        cols = pl.ds(c * share * width, share * width)
        for i, (source, target) in enumerate(
            ((velocity_ref, velocity_out), (affine_ref, affine_out))
        ):
            copy = pltpu.make_async_copy(
                source.at[:, cols], target.at[:, cols], sems.at[i + 1, c]
            )
            copy.start()
            copies.append(copy)
    for copy in copies:
        copy.wait()


def unpack(dest, count, returned, grid, width):
    particles = dest.shape[0] * width
    velocity = jax.ShapeDtypeStruct((3, particles), F32)
    affine = jax.ShapeDtypeStruct((9, particles), F32)
    return pl.pallas_call(
        unpack_kernel,
        name="unpack",
        out_shape=(velocity, affine, jax.ShapeDtypeStruct(grid.shape, F32)),
        in_specs=[SMEM, SMEM, VMEM, VMEM],
        out_specs=(HBM, HBM, HBM),
        scratch_shapes=[
            pltpu.VMEM(velocity.shape, F32),
            pltpu.VMEM(affine.shape, F32),
            pltpu.SemaphoreType.DMA((3, PARTS)),
        ],
        compiler_params=pltpu.CompilerParams(vmem_limit_bytes=20 << 20),
    )(dest, count, returned, grid)


def per_device(
    particle_mass,
    particle_velocity,
    particle_affine,
    particle_cell,
    particle_fraction,
    block_owner,
    block_slot,
    block_count,
    cell_drag,
):
    group = lax.axis_size(GROUP_AXES)
    blocks = block_count.shape[0]
    width = particle_mass.shape[0] // blocks
    cap = max(1, 2 * blocks // group)
    subs = min(cap, PARTS)
    packed, dest, marks = pack(
        cap,
        group,
        block_owner[:, 0],
        block_slot,
        block_count,
        particle_mass.reshape(blocks, 1, width),
        particle_velocity,
        particle_affine,
        particle_cell,
        particle_fraction,
    )
    arrived, deposits, told = scatter(cap, subs, packed, marks)
    ratio, rounded = grid_step(cap, told, deposits, cell_drag)
    returned, grid = gather(cap, subs, told, arrived, rounded, ratio)
    new_velocity, new_affine, grid_velocity = unpack(dest, block_count, returned, grid, width)
    return jnp.transpose(grid_velocity, (1, 0, 2)), new_velocity, new_affine


def solution(mesh):
    everywhere = ("gx", "gy", "gz")
    return jax.shard_map(
        per_device,
        mesh=mesh,
        in_specs=(
            P(everywhere),
            P(None, everywhere),
            P(None, everywhere),
            P(None, everywhere),
            P(None, everywhere),
            P(everywhere, None),
            P(everywhere),
            P(everywhere),
            P(everywhere, None),
        ),
        out_specs=(P(everywhere, None, None), P(None, everywhere), P(None, everywhere)),
        check_vma=False,
    )
```

```python
import functools

import jax
import jax.numpy as jnp
from jax import lax
from jax.experimental import pallas as pl
from jax.experimental.pallas import tpu as pltpu
from jax.sharding import PartitionSpec as P

EDGE = 16
QUANT = 1024
LANES = 128
FIELDS = 16
RESULTS = 12
PARTS = 4
UNROLL = 4
GROUP_AXES = ("gy", "gz")
F32 = jnp.float32
BF16 = jnp.bfloat16
MESH = pl.DeviceIdType.MESH


SMEM = pl.BlockSpec(memory_space=pltpu.SMEM)
VMEM = pl.BlockSpec(memory_space=pltpu.VMEM)
HBM = pl.BlockSpec(memory_space=pltpu.HBM)


def cost(flops):
    return pl.CostEstimate(flops=flops, bytes_accessed=1 << 22, transcendentals=0)


def twice(rows):
    return jnp.concatenate([rows, rows], axis=0)


def span_of(part):
    return slice(part * LANES, (part + 1) * LANES)


def encode(code):
    power = code >> 8
    scale = jnp.where(
        power < 28,
        (1 << (power & 31)).astype(F32),
        (1 << jnp.maximum(power - 28, 0)).astype(F32) * 2.0**28,
    )
    size = ((code & 127) + 128).astype(F32) * (scale * 2.0**-28)
    return jnp.where((code & 128) != 0, -size, size)


def pack_kernel(
    cap,
    owner_ref,
    slot_ref,
    count_ref,
    mass_ref,
    velocity_ref,
    affine_ref,
    cell_ref,
    fraction_ref,
    packed_ref,
    dest_ref,
    marks_ref,
    used_ref,
    tile_ref,
    stage_ref,
    mass_v,
    velocity_v,
    affine_v,
    cell_v,
    fraction_v,
    load_sems,
):
    sources = (mass_ref, velocity_ref, affine_ref, cell_ref, fraction_ref)
    staged = (mass_v, velocity_v, affine_v, cell_v, fraction_v)
    blocks, _, width = mass_v.shape
    share = blocks // PARTS
    loads = []
    for c in range(PARTS):
        rows = pl.ds(c * share, share)
        cols = pl.ds(c * share * width, share * width)
        for i, (source, target) in enumerate(zip(sources, staged)):
            part = rows if i == 0 else (slice(None), cols)
            loads.append(
                pltpu.make_async_copy(source.at[part], target.at[part], load_sems.at[i, c])
            )
    for load in loads:
        load.start()
    group = used_ref.shape[0]
    quarters = width // LANES
    rows = quarters * FIELDS

    def clear_used(i, carry):
        used_ref[i] = 0
        return carry

    def clear_slots(i, carry):
        tile_ref[i] = -1
        packed_ref[i] = jnp.zeros((rows, LANES), BF16)
        return carry

    lax.fori_loop(0, group, clear_used, 0, unroll=8)
    lax.fori_loop(0, group * cap, clear_slots, 0, unroll=8)

    def place(block, carry):
        owner = owner_ref[block]
        rank = used_ref[owner]
        used_ref[owner] = rank + 1
        where = owner * cap + rank
        tile_ref[where] = slot_ref[block]
        dest_ref[block] = where
        return carry

    lax.fori_loop(0, blocks, place, 0, unroll=2)
    lane = lax.broadcasted_iota(jnp.int32, (1, LANES), 1)

    def mark(owner, carry):
        row = jnp.full((1, LANES), -1, jnp.int32)
        for i in range(cap):
            row = jnp.where(lane == i, tile_ref[owner * cap + i], row)
        marks_ref[owner] = row
        return carry

    lax.fori_loop(0, group, mark, 0, unroll=2)
    place_lane = lax.broadcasted_iota(jnp.int32, (1, width), 1)

    def pack(step, carry):
        for u in range(UNROLL):
            block = step * UNROLL + u
            cols = pl.ds(pl.multiple_of(block * width, LANES), width)
            live = jnp.where(place_lane < count_ref[block], mass_v[block], 0.0)
            velocity = velocity_v[:, cols]
            affine = affine_v[:, cols]
            code = encode(cell_v[:, cols] * QUANT + fraction_v[:, cols])
            for q in range(quarters):
                base = u * rows + q * FIELDS
                stage_ref[base : base + 1] = live[:, span_of(q)]
                stage_ref[base + 1 : base + 4] = velocity[:, span_of(q)]
                stage_ref[base + 4 : base + 13] = affine[:, span_of(q)]
                stage_ref[base + 13 : base + 16] = code[:, span_of(q)]
        for u in range(UNROLL):
            packed_ref[dest_ref[step * UNROLL + u]] = stage_ref[
                u * rows : (u + 1) * rows
            ].astype(BF16)
        return carry

    for c in range(PARTS):
        for load in loads[c * len(sources) : (c + 1) * len(sources)]:
            load.wait()
        lax.fori_loop(c * share // UNROLL, (c + 1) * share // UNROLL, pack, 0)


def pack(cap, group, owner, slot, count, mass, velocity, affine, cell, fraction):
    slots = group * cap
    blocks, _, width = mass.shape
    rows = width // LANES * FIELDS
    arrays = (mass, velocity, affine, cell, fraction)
    return pl.pallas_call(
        functools.partial(pack_kernel, cap),
        name="pack",
        out_shape=(
            pltpu.VMEM((slots, rows, LANES), BF16),
            jax.ShapeDtypeStruct(owner.shape, jnp.int32),
            pltpu.VMEM((group, 1, LANES), jnp.int32),
        ),
        in_specs=[SMEM] * 3 + [HBM] * 5,
        out_specs=(VMEM, SMEM, VMEM),
        scratch_shapes=[
            pltpu.SMEM((group,), jnp.int32),
            pltpu.SMEM((slots,), jnp.int32),
            pltpu.VMEM((UNROLL * rows, LANES), F32),
        ]
        + [pltpu.VMEM(array.shape, array.dtype) for array in arrays]
        + [pltpu.SemaphoreType.DMA((len(arrays), PARTS))],
        compiler_params=pltpu.CompilerParams(vmem_limit_bytes=60 << 20),
    )(owner, slot, count, *arrays)


class Group:
    def __init__(self):
        self.wide = lax.axis_size(GROUP_AXES[1])
        self.size = lax.axis_size(GROUP_AXES)
        self.me = lax.axis_index(GROUP_AXES[0]) * self.wide + lax.axis_index(GROUP_AXES[1])

    def device(self, peer):
        return {GROUP_AXES[0]: peer // self.wide, GROUP_AXES[1]: peer % self.wide}

    def greet(self):
        barrier = pltpu.get_barrier_semaphore()

        def signal(k, carry):
            pl.semaphore_signal(
                barrier, inc=1, device_id=self.device(self.me ^ k), device_id_type=MESH
            )
            return carry

        lax.fori_loop(1, self.size, signal, 0)

    def gathered(self):
        pl.semaphore_wait(pltpu.get_barrier_semaphore(), self.size - 1)


def decode(value):
    size = jnp.abs(value)
    position = jnp.where(value < 0.0, 128.0 / QUANT, 0.0)
    for bit in (32, 16, 8, 4, 2, 1):
        large = size >= 2.0 ** (7 + bit - 28)
        size = jnp.where(large, size * 2.0**-bit, size)
        position = jnp.where(large, position + bit * 256.0 / QUANT, position)
    return position + (size * (2.0**28 / QUANT) + (0.5 + 0.5 / QUANT - 128.0 / QUANT))


def load_item(u, item_ref, fields_ref):
    rows = item_ref.shape[0]
    first = u * rows
    fields_ref[first : first + rows] = item_ref[...].astype(F32)
    for q in range(rows // FIELDS):
        base = first + q * FIELDS
        fields_ref[base + 13 : base + 16] = decode(fields_ref[base + 13 : base + 16])

    def spread(field, part):
        return twice(
            jnp.concatenate(
                [
                    jnp.broadcast_to(fields_ref[pl.ds(row, 1), :], (8, LANES))
                    for row in (
                        first + (part * 2) * FIELDS + field,
                        first + (part * 2 + 1) * FIELDS + field,
                    )
                ],
                axis=1,
            )
        )

    return spread


def stencil(position, node):
    offset = node - position
    magnitude = jnp.abs(offset)
    outer_part = jnp.maximum(1.5 - magnitude, 0.0)
    weight = jnp.where(
        magnitude < 0.5, 0.75 - magnitude * magnitude, 0.5 * outer_part * outer_part
    )
    return weight, weight * offset


def planes(u, spread, part, node, rows_ref):
    factors_y = stencil(spread(14, part), node)
    factors_z = [factor.astype(BF16) for factor in stencil(spread(15, part), node)]
    firsts = [((u * 2 + part) * 2 + k) * 2 * EDGE for k in range(2)]
    for first, factor in zip(firsts, factors_y):
        for q in range(2):
            rows_ref[first + q * EDGE : first + (q + 1) * EDGE] = factor[:, span_of(q)]

    def row(first, y):
        return jnp.concatenate(
            [
                twice(
                    jnp.broadcast_to(rows_ref[pl.ds(first + q * EDGE + y, 1), :], (8, LANES))
                ).astype(BF16)
                for q in range(2)
            ],
            axis=1,
        )

    zero, one, two = [], [], []
    for y in range(EDGE):
        weight_row, slope_row = row(firsts[0], y), row(firsts[1], y)
        zero.append(weight_row * factors_z[0])
        one.append(slope_row * factors_z[0])
        two.append(weight_row * factors_z[1])
    return [jnp.concatenate(parts, axis=0) for parts in (zero, one, two)]


def nodes():
    return lax.broadcasted_iota(jnp.int32, (EDGE, 2 * LANES), 0).astype(F32)


def deposit(u, item_ref, fields_ref, rows_ref):
    spread = load_item(u, item_ref, fields_ref)
    node = nodes()
    total = None
    for part in range(item_ref.shape[0] // (2 * FIELDS)):
        weight_x, slope_x = stencil(spread(13, part), node)
        mass = spread(0, part)
        mass_x = mass * weight_x
        mass_slope = mass * slope_x
        nothing = jnp.zeros(mass_x.shape, BF16)
        lead_zero, lead_one, lead_two = [mass_x.astype(BF16)], [nothing], [nothing]
        for d in range(3):
            lead_zero.append(
                (spread(1 + d, part) * mass_x + spread(4 + 3 * d, part) * mass_slope).astype(BF16)
            )
            lead_one.append((spread(5 + 3 * d, part) * mass_x).astype(BF16))
            lead_two.append((spread(6 + 3 * d, part) * mass_x).astype(BF16))
        lead = jnp.concatenate(
            [jnp.concatenate(rows, axis=0) for rows in (lead_zero, lead_one, lead_two)], axis=1
        )
        plane = jnp.concatenate(planes(u, spread, part, node, rows_ref), axis=1)
        sums = lax.dot_general(
            lead, plane, (((1,), (1,)), ((), ())), preferred_element_type=F32
        )
        total = sums if total is None else total + sums
    return total


def interpolate(u, item_ref, grid_rows, fields_ref, rows_ref, parts_ref):
    spread = load_item(u, item_ref, fields_ref)
    node = nodes()
    quarters = item_ref.shape[0] // FIELDS
    first = u * quarters * RESULTS * 8
    for part in range(quarters // 2):
        weight_x, slope_x = stencil(spread(13, part), node)
        moments = [
            jnp.dot(grid_rows, plane, preferred_element_type=F32)
            for plane in planes(u, spread, part, node, rows_ref)
        ]
        slope_four = 4.0 * slope_x
        weight_four = 4.0 * weight_x
        for d in range(3):
            span = slice(d * EDGE, (d + 1) * EDGE)
            entries = (
                (d, weight_x, moments[0]),
                (3 + 3 * d, slope_four, moments[0]),
                (4 + 3 * d, weight_four, moments[1]),
                (5 + 3 * d, weight_four, moments[2]),
            )
            for entry, factor, moment in entries:
                product = factor * moment[span]
                partial = product[:8] + product[8:]
                for q in range(2):
                    at = first + ((part * 2 + q) * RESULTS + entry) * 8
                    parts_ref[at : at + 8] = partial[:, span_of(q)]
    groups = []
    for g in range(quarters * RESULTS // 8):
        total = parts_ref[pl.ds(first + g * 64, 8, stride=8), :]
        for j in range(1, 8):
            total = total + parts_ref[pl.ds(first + g * 64 + j, 8, stride=8), :]
        groups.append(total)
    return jnp.concatenate(groups, axis=0).astype(BF16)


def scatter_kernel(
    cap,
    subs,
    packed_ref,
    marks_ref,
    arrived_ref,
    sums_ref,
    told_ref,
    fields_ref,
    rows_ref,
    send_sems,
    recv_sems,
    mark_send,
    mark_recv,
):
    group = Group()
    n, me = group.size, group.me
    per = cap // subs
    group.greet()

    def rows_of(device, sub):
        return pl.ds(device * cap + sub * per, per)

    def transfer(k, sub):
        peer = me ^ k
        return pltpu.make_async_remote_copy(
            src_ref=packed_ref.at[rows_of(peer, sub)],
            dst_ref=arrived_ref.at[rows_of(me, sub)],
            send_sem=send_sems.at[k, sub],
            recv_sem=recv_sems.at[k, sub],
            device_id=group.device(peer),
            device_id_type=MESH,
        )

    def arrival(k, sub):
        rows = rows_of(me ^ k, sub)
        return pltpu.make_async_copy(
            packed_ref.at[rows], arrived_ref.at[rows], recv_sems.at[k, sub]
        )

    def mark_transfer(k):
        peer = me ^ k
        return pltpu.make_async_remote_copy(
            src_ref=marks_ref.at[peer],
            dst_ref=told_ref.at[me],
            send_sem=mark_send.at[k],
            recv_sem=mark_recv.at[k],
            device_id=group.device(peer),
            device_id_type=MESH,
        )

    own_marks = pltpu.make_async_copy(marks_ref.at[me], told_ref.at[me], mark_recv.at[0])
    own_marks.start()

    for sub in range(subs):
        arrival(0, sub).start()
    group.gathered()
    half = n // 2

    def send_near(step, carry):
        transfer(1 + step // subs, step % subs).start()
        return carry

    def send_far(step, carry):
        transfer(half + step % half, step // half).start()
        return carry

    def send_marks(k, carry):
        mark_transfer(k).start()
        return carry

    lax.fori_loop(0, (half - 1) * subs, send_near, 0)
    lax.fori_loop(0, half * subs, send_far, 0)
    lax.fori_loop(1, n, send_marks, 0)
    pair = 2
    strides = half // pair

    def take(step, carry):
        side = step // (strides * subs)
        rest = step % (strides * subs)
        sub = (1 - side) * (rest % subs) + side * (rest // strides)
        first = side * half + pair * ((1 - side) * (rest // subs) + side * (rest % strides))
        for j in range(pair):
            arrival(first + j, sub).wait()
        for j in range(pair):
            for i in range(per):
                slot = (me ^ (first + j)) * cap + sub * per + i
                sums_ref[slot] = deposit(
                    j * per + i, arrived_ref.at[slot], fields_ref, rows_ref
                )
        return carry

    lax.fori_loop(0, strides * subs * 2, take, 0)
    own_marks.wait()

    def settle(k, carry):
        mark_transfer(k).wait_recv()
        mark_transfer(k).wait_send()
        for sub in range(subs):
            transfer(k, sub).wait_send()
        return carry

    lax.fori_loop(1, n, settle, 0)


def scatter(cap, subs, packed, marks):
    slots, rows, _ = packed.shape
    group = marks.shape[0]
    quarters = rows // FIELDS
    unroll = 2 * (cap // subs)
    return pl.pallas_call(
        functools.partial(scatter_kernel, cap, subs),
        name="scatter_step",
        out_shape=(
            jax.ShapeDtypeStruct(packed.shape, BF16),
            jax.ShapeDtypeStruct((slots, 4 * EDGE, EDGE * EDGE), F32),
            jax.ShapeDtypeStruct(marks.shape, jnp.int32),
        ),
        in_specs=[VMEM, VMEM],
        out_specs=(VMEM,) * 3,
        scratch_shapes=[
            pltpu.VMEM((unroll * rows, LANES), F32),
            pltpu.VMEM((unroll * 2 * quarters * EDGE, LANES), F32),
            pltpu.SemaphoreType.DMA((group, subs)),
            pltpu.SemaphoreType.DMA((group, subs)),
            pltpu.SemaphoreType.DMA((group,)),
            pltpu.SemaphoreType.DMA((group,)),
        ],
        compiler_params=pltpu.CompilerParams(
            collective_id=0, has_side_effects=True, vmem_limit_bytes=30 << 20
        ),
        cost_estimate=cost(10**10),
    )(packed, marks)


def grid_kernel(cap, told_ref, deposits_ref, drag_ref, ratio_ref, round_ref, sums_ref):
    plane_size = EDGE * EDGE
    tiles = drag_ref.shape[0]

    def start(t, carry):
        for x in range(EDGE):
            sums_ref[t, x : x + 1, :] = drag_ref[
                pl.ds(t, 1), x * plane_size : (x + 1) * plane_size
            ]
        sums_ref[t, EDGE:, :] = jnp.zeros((3 * EDGE, plane_size), F32)
        return carry

    lax.fori_loop(0, tiles, start, 0, unroll=2)
    sums_ref[tiles] = jnp.zeros((4 * EDGE, plane_size), F32)

    def add(device, carry):
        for i in range(cap):
            mark = told_ref[device, 0, i]
            tile = jnp.where(mark < 0, tiles, mark)
            sums_ref[tile] += deposits_ref[device * cap + i]
        return carry

    lax.fori_loop(0, told_ref.shape[0], add, 0)

    def divide(t, carry):
        mass = sums_ref[t, :EDGE, :]
        ratio = jnp.concatenate(
            [sums_ref[t, (d + 1) * EDGE : (d + 2) * EDGE, :] / mass for d in range(3)], axis=0
        )
        ratio_ref[t] = ratio
        round_ref[t] = ratio.astype(BF16)
        return carry

    lax.fori_loop(0, tiles, divide, 0, unroll=2)


def grid_step(cap, told, deposits, drag):
    tiles = drag.shape[0]
    plane_size = EDGE * EDGE
    return pl.pallas_call(
        functools.partial(grid_kernel, cap),
        name="grid_step",
        out_shape=(
            pltpu.VMEM((tiles, 3 * EDGE, plane_size), F32),
            pltpu.VMEM((tiles, 3 * EDGE, plane_size), BF16),
        ),
        in_specs=[SMEM, VMEM, VMEM],
        out_specs=(VMEM, VMEM),
        scratch_shapes=[pltpu.VMEM((tiles + 1, 4 * EDGE, plane_size), F32)],
        compiler_params=pltpu.CompilerParams(vmem_limit_bytes=20 << 20),
        cost_estimate=cost(10**9),
    )(told, deposits, drag)


def gather_kernel(
    cap,
    subs,
    told_ref,
    arrived_ref,
    round_ref,
    ratio_ref,
    returned_ref,
    grid_ref,
    results_ref,
    fields_ref,
    rows_ref,
    parts_ref,
    send_sems,
    recv_sems,
):
    group = Group()
    n, me = group.size, group.me
    per = cap // subs
    group.greet()

    def rows_of(device, sub):
        return pl.ds(device * cap + sub * per, per)

    def transfer(k, sub):
        peer = me ^ k
        return pltpu.make_async_remote_copy(
            src_ref=results_ref.at[rows_of(peer, sub)],
            dst_ref=returned_ref.at[rows_of(me, sub)],
            send_sem=send_sems.at[k, sub],
            recv_sem=recv_sems.at[k, sub],
            device_id=group.device(peer),
            device_id_type=MESH,
        )

    def arrival(k, sub):
        rows = rows_of(me ^ k, sub)
        return pltpu.make_async_copy(
            results_ref.at[rows], returned_ref.at[rows], recv_sems.at[k, sub]
        )

    pair = 2
    half = n // 2
    strides = half // pair

    def place(step):
        side = step // (strides * subs)
        rest = step % (strides * subs)
        return n - 1 - side * half - (rest % strides) * pair, rest // strides

    def work(step):
        top, sub = place(step)
        for j in range(pair):
            source = me ^ (top - j)
            for i in range(per):
                slot = source * cap + sub * per + i
                tile = jnp.maximum(told_ref[source, 0, sub * per + i], 0)
                results_ref[slot] = interpolate(
                    j * per + i,
                    arrived_ref.at[slot],
                    round_ref[tile],
                    fields_ref,
                    rows_ref,
                    parts_ref,
                )

    def send(step):
        top, sub = place(step)
        for j in range(pair):
            k = top - j

            @pl.when(k != 0)
            def _():
                transfer(k, sub).start()

            @pl.when(k == 0)
            def _():
                arrival(0, sub).start()

    steps = half // pair * subs * 2
    work(0)
    group.gathered()
    send(0)

    def work_and_send(step, carry):
        work(step)

        @pl.when(step > 1)
        def _():
            send(step - 1)

        return carry

    lax.fori_loop(1, steps, work_and_send, 0)
    send(steps - 1)

    plane_size = EDGE * EDGE

    def spread_rows(t, carry):
        for d in range(3):
            for x in range(EDGE):
                row = d * EDGE + x
                grid_ref[d, pl.ds(t, 1), x * plane_size : (x + 1) * plane_size] = ratio_ref[
                    t, row : row + 1, :
                ]
        return carry

    lax.fori_loop(0, ratio_ref.shape[0], spread_rows, 0)

    def settle(k, carry):
        for sub in range(subs):
            transfer(k, sub).wait_recv()
            transfer(k, sub).wait_send()
        return carry

    for sub in range(subs):
        arrival(0, sub).wait()
    lax.fori_loop(1, n, settle, 0)


def gather(cap, subs, told, arrived, rounded, ratio):
    slots, rows, _ = arrived.shape
    group = told.shape[0]
    quarters = rows // FIELDS
    unroll = 2 * (cap // subs)
    result = (slots, quarters * RESULTS, LANES)
    return pl.pallas_call(
        functools.partial(gather_kernel, cap, subs),
        name="gather_step",
        out_shape=(
            pltpu.VMEM(result, BF16),
            pltpu.VMEM((3, ratio.shape[0], EDGE**3), F32),
        ),
        in_specs=[SMEM, VMEM, VMEM, VMEM],
        out_specs=(VMEM, VMEM),
        scratch_shapes=[
            pltpu.VMEM(result, BF16),
            pltpu.VMEM((unroll * rows, LANES), F32),
            pltpu.VMEM((unroll * 2 * quarters * EDGE, LANES), F32),
            pltpu.VMEM((unroll * quarters * RESULTS * 8, LANES), F32),
            pltpu.SemaphoreType.DMA((group, subs)),
            pltpu.SemaphoreType.DMA((group, subs)),
        ],
        compiler_params=pltpu.CompilerParams(
            collective_id=1, has_side_effects=True, vmem_limit_bytes=40 << 20
        ),
        cost_estimate=cost(10**10),
    )(told, arrived, rounded, ratio)


def unpack_kernel(
    dest_ref,
    count_ref,
    returned_ref,
    grid_ref,
    velocity_out,
    affine_out,
    grid_out,
    velocity_ref,
    affine_ref,
    sems,
):
    copies = [pltpu.make_async_copy(grid_ref, grid_out, sems.at[0, 0])]
    copies[0].start()
    blocks = dest_ref.shape[0]
    width = velocity_ref.shape[1] // blocks
    lane = lax.broadcasted_iota(jnp.int32, (1, LANES), 1)

    def unpack(block, carry):
        count = count_ref[block]
        rows = returned_ref[dest_ref[block]].astype(F32)
        for q in range(width // LANES):
            first = q * LANES
            cols = pl.ds(pl.multiple_of(block * width + first, LANES), LANES)
            part = jnp.where(lane + first < count, rows[q * RESULTS : (q + 1) * RESULTS], 0.0)
            velocity_ref[:, cols] = part[:3]
            affine_ref[:, cols] = part[3:]
        return carry

    share = blocks // PARTS
    for c in range(PARTS):
        lax.fori_loop(c * share, (c + 1) * share, unpack, 0, unroll=4)
        cols = pl.ds(c * share * width, share * width)
        for i, (source, target) in enumerate(
            ((velocity_ref, velocity_out), (affine_ref, affine_out))
        ):
            copy = pltpu.make_async_copy(
                source.at[:, cols], target.at[:, cols], sems.at[i + 1, c]
            )
            copy.start()
            copies.append(copy)
    for copy in copies:
        copy.wait()


def unpack(dest, count, returned, grid, width):
    particles = dest.shape[0] * width
    velocity = jax.ShapeDtypeStruct((3, particles), F32)
    affine = jax.ShapeDtypeStruct((9, particles), F32)
    return pl.pallas_call(
        unpack_kernel,
        name="unpack",
        out_shape=(velocity, affine, jax.ShapeDtypeStruct(grid.shape, F32)),
        in_specs=[SMEM, SMEM, VMEM, VMEM],
        out_specs=(HBM, HBM, HBM),
        scratch_shapes=[
            pltpu.VMEM(velocity.shape, F32),
            pltpu.VMEM(affine.shape, F32),
            pltpu.SemaphoreType.DMA((3, PARTS)),
        ],
        compiler_params=pltpu.CompilerParams(vmem_limit_bytes=20 << 20),
    )(dest, count, returned, grid)


def per_device(
    particle_mass,
    particle_velocity,
    particle_affine,
    particle_cell,
    particle_fraction,
    block_owner,
    block_slot,
    block_count,
    cell_drag,
):
    group = lax.axis_size(GROUP_AXES)
    blocks = block_count.shape[0]
    width = particle_mass.shape[0] // blocks
    cap = max(1, 2 * blocks // group)
    subs = min(cap, PARTS)
    packed, dest, marks = pack(
        cap,
        group,
        block_owner[:, 0],
        block_slot,
        block_count,
        particle_mass.reshape(blocks, 1, width),
        particle_velocity,
        particle_affine,
        particle_cell,
        particle_fraction,
    )
    arrived, deposits, told = scatter(cap, subs, packed, marks)
    ratio, rounded = grid_step(cap, told, deposits, cell_drag)
    returned, grid = gather(cap, subs, told, arrived, rounded, ratio)
    new_velocity, new_affine, grid_velocity = unpack(dest, block_count, returned, grid, width)
    return jnp.transpose(grid_velocity, (1, 0, 2)), new_velocity, new_affine


def solution(mesh):
    everywhere = ("gx", "gy", "gz")
    return jax.shard_map(
        per_device,
        mesh=mesh,
        in_specs=(
            P(everywhere),
            P(None, everywhere),
            P(None, everywhere),
            P(None, everywhere),
            P(None, everywhere),
            P(everywhere, None),
            P(everywhere),
            P(everywhere),
            P(everywhere, None),
        ),
        out_specs=(P(everywhere, None, None), P(None, everywhere), P(None, everywhere)),
        check_vma=False,
    )
```
